32 devices in a mesh: groups: 2 (over y), expert: 8 (over z, core), tensor: 2 (over x).
Axes of the slice: x: 2, y: 2, z: 4, core: 2. Of those that a mesh axis runs over, the one named last changes fastest.
Arguments:
- query: bfloat16 [768, 8192], P(('groups', 'expert'), 'tensor'), parts along dimension 0, may hold values from -40 to 40
- latest_key_value: bfloat16 [768, 2, 512], P(('groups', 'expert'), None, 'tensor'), parts along dimension 0, may hold values from -6 to 6
- cache: bfloat16 [768, 2, 128, 512], P(('groups', 'expert'), None, None, 'tensor'), parts along dimension 0, may hold values from -6 to 6
- lengths: int32 [768], P(('groups', 'expert')), parts along dimension 0, may hold values from 2 to 128
- w_out: bfloat16 [8192, 4096], P('tensor', 'expert'), may hold values from -0.0625 to 0.0625
- residual_in: bfloat16 [768, 4096], P(('groups', 'expert', 'tensor')), parts along dimension 0, may hold values from -6 to 6
- norm_gain: bfloat16 [4096], replicated, may hold values from 0.5 to 1.5
- expert_ids: int32 [768, 8], P(('groups', 'expert')), parts along dimension 0, may hold values from 0 to 15, all different within a row; in each aligned block of 48 rows (0 to 47, 48 to 95, ...) at most 48 rows name the same one
- route_weights: float32 [768, 8], P(('groups', 'expert')), parts along dimension 0, may hold values from 0.05 to 0.5
- w_gate: bfloat16 [16, 4096, 768], P('expert', None, 'tensor'), may hold values from -0.09375 to 0.09375
- w_up: bfloat16 [16, 4096, 768], P('expert', None, 'tensor'), may hold values from -0.09375 to 0.09375
- w_down: bfloat16 [16, 768, 4096], P('expert', 'tensor'), may hold values from -0.21875 to 0.21875
Outputs:
- layer_out: bfloat16 [768, 4096], P(('groups', 'expert', 'tensor')), parts along dimension 0
The draws below stay inside these ranges and needn't reach their ends.
There are 2 independent parts, one for each index of `groups`. The reference program is written for one: setup_inputs(seed, part) draws one part's arguments, and reference() takes and returns one part's arrays. A program takes and returns all parts, laid end to end along the dimension named above; an argument that names none is the same for every part. Nothing has to cross between parts.
Inputs may be any that keep to these rules, and one draw needn't show every extreme that they name: `expert_ids`: the 8 entries of a row differ. Within each aligned block of 48 rows (the rows of one index of the expert axis) no expert is named by more than 48 rows, and in every draw some block reaches that bound.
All inputs are finite; a program needn't handle non-finite values.
Results may differ from the reference program's by a relative error of at most 0.0095.
Values may be sent and summed in bfloat16 or wider, within the bound.
A program may use at most 128 MiB of HBM per device.

```python
import math
import jax
import jax.numpy as jnp
import numpy as np
from jax import lax

D = 4096
QUERY_HEADS = 64
KEY_VALUE_HEADS = 4
HEAD_SIZE = 128
TOP = 8
FF = 768
TOK_DEV = 48
CACHE_LENGTH = 128
EXPERTS = 16
REQUEST_TOTAL = 384
CAP = 48
N_TENSOR = 2


def cache_values(key):
    folded = jax.random.fold_in(key, 17)
    tensor_dims = (REQUEST_TOTAL, 2, CACHE_LENGTH, KEY_VALUE_HEADS * HEAD_SIZE)
    values = jnp.clip(jax.random.normal(folded, tensor_dims, jnp.float32), -6.0, 6.0)
    return values


def draw_cache(key, part):
    return cache_values(key).astype(jnp.bfloat16)


def draw_query(key, part):
    folded = jax.random.fold_in(key, 29)
    tensor_dims = (REQUEST_TOTAL, QUERY_HEADS * HEAD_SIZE)
    values = jnp.clip(jax.random.normal(folded, tensor_dims, jnp.float32), -6.0, 6.0)
    return values.astype(jnp.bfloat16)


def set_ends(result, stream_key, low, top_value):
    longest = result.shape.index(max(result.shape))
    spots = []
    for shift in (0, 1):
        where = [jax.random.randint(jax.random.fold_in(stream_key, axis), (), 0, length) for axis, length in enumerate(result.shape)]
        where[longest] = (where[longest] + shift) % result.shape[longest]
        spots.append(tuple(where))
    return result.at[spots[0]].set(low).at[spots[1]].set(top_value)


def level_of(own_key, dims, pieces, smallest, top_value):
    level = 1.0
    for axis_at, shards_of in pieces:
        draws = jax.random.uniform(jax.random.fold_in(jax.random.fold_in(own_key, 6), axis_at), (shards_of,), jnp.float32, smallest / len(pieces), top_value / len(pieces))
        level = level * jnp.repeat(jnp.exp(draws), dims[axis_at] // shards_of).reshape((-1,) + (1,) * (len(dims) - 1 - axis_at))
    return level


def routed_block(stream_key, own, number, rows, count, top, bound, slope):
    sequence = jax.random.permutation(stream_key, count)
    heavy_load, ordinary = shares(count, rows * top, bound, slope, True), shares(count, rows * top, bound, slope, False)
    places = jnp.arange(count)

    def named(sizes, turn):
        used = int((sizes > 0).sum())
        fixed = max(1, used // 4)
        shifted = fixed + (places - fixed + turn * (used - fixed)) % max(1, count - fixed)
        return jnp.zeros((count,), jnp.int32).at[sequence[jnp.where(places < fixed, places, shifted)]].set(jnp.asarray(sizes, jnp.int32))

    sizes = jnp.where(number % 4 == 0, named(heavy_load, number // 4), named(ordinary, number - number // 4 - 1))
    mixed = jax.random.permutation(jax.random.fold_in(own, 3), count)
    donor, taker = mixed[0:count // 2 * 2:2], mixed[1:count // 2 * 2:2]
    slack = jnp.minimum(sizes[donor] - 1, bound - sizes[taker]) // 2
    slack = jnp.where((donor == sequence[0]) | (taker == sequence[0]) | (sizes[taker] == 0), 0, jnp.maximum(slack, 0))
    shifted = jax.random.randint(jax.random.fold_in(own, 4), (count // 2,), 0, 1 << 20) % (slack + 1)
    sizes = sizes.at[donor].add(-shifted).at[taker].add(shifted)
    items = jnp.searchsorted(jnp.cumsum(sizes), jnp.arange(rows * top), side="right").astype(jnp.int32)
    table = items.reshape(top, rows).T
    table = table[jax.random.permutation(jax.random.fold_in(own, 1), rows)]
    turn = jax.random.randint(jax.random.fold_in(own, 2), (rows, 1), 0, top)
    return jnp.take_along_axis(table, (jnp.arange(top)[None, :] + turn) % top, axis=1)


def shares(count, total, most, slope, full):
    weights = [(1 << 20) // math.isqrt(rank ** slope) + 1 for rank in range(1, count + 1)]
    largest = most if full else min(most, max(-(-total // count), total * weights[0] // sum(weights)))
    least = 1 if total - largest >= count - 1 else 0
    counts, spare = [largest] + [least] * (count - 1), total - largest - least * (count - 1)
    while spare > 0:
        movable = [i for i in range(1, count) if counts[i] < largest] or [i for i in range(1, count) if counts[i] < most]
        whole, budget = sum([weights[i] for i in movable]), spare
        for i in movable:
            more = min(most - counts[i], max(1, budget * weights[i] // whole), spare)
            counts[i] = counts[i] + more
            spare = spare - more
    return np.array(counts)


def centred(stream_key, dims, width, bound, cuts=(), held_as=jnp.bfloat16):
    values = width * jax.random.normal(stream_key, dims, jnp.float32)
    if cuts:
        values = values * level_of(stream_key, dims, cuts, -0.22, 0.18)
    return jnp.clip(values, -bound, bound).astype(held_as)


def setup_inputs(seed: int = 0, part: int = 0) -> dict:
    splits = jax.random.split(jax.random.key(seed), 13)
    part_splits = jax.random.split(jax.random.fold_in(splits[12], part), 13)
    query = draw_query(jax.random.fold_in(jax.random.fold_in(splits[12], part), 71), part)
    latest_key_value = centred(part_splits[1], (REQUEST_TOTAL, 2, KEY_VALUE_HEADS * HEAD_SIZE), 1.0, 6.0, ((0, 8), (2, 2)))
    cache = draw_cache(jax.random.fold_in(jax.random.fold_in(splits[12], part), 71), part)
    lengths = set_ends(jax.random.randint(part_splits[3], (REQUEST_TOTAL,), 2, CACHE_LENGTH + 1), jax.random.fold_in(part_splits[3], 1), 2, CACHE_LENGTH).astype(jnp.int32)
    w_out = centred(splits[4], (QUERY_HEADS * HEAD_SIZE, D), (QUERY_HEADS * HEAD_SIZE) ** -0.5, 0.0625, ((0, 2), (1, 8)))
    residual_in = centred(part_splits[5], (REQUEST_TOTAL, D), 1.0, 6.0, ((0, 16),))
    norm_gain = jnp.clip(1.0 + 0.1 * jax.random.normal(splits[6], (D,), jnp.float32), 0.5, 1.5).astype(jnp.bfloat16)
    expert_ids_keys = jax.random.split(jax.random.fold_in(part_splits[7], 1), REQUEST_TOTAL // TOK_DEV)
    expert_ids_turns = jax.random.permutation(jax.random.fold_in(part_splits[7], 3), REQUEST_TOTAL // TOK_DEV)
    expert_ids = jax.vmap(lambda own, number: routed_block(jax.random.fold_in(part_splits[7], 2), own, number, TOK_DEV, EXPERTS, TOP, CAP, 2))(expert_ids_keys, expert_ids_turns).reshape((REQUEST_TOTAL, TOP))
    route_weights = jnp.clip(jnp.exp(math.log(0.5) - 2.3025851 * jax.random.uniform(part_splits[8], (REQUEST_TOTAL, TOP), jnp.float32) ** level_of(part_splits[8], (REQUEST_TOTAL, TOP), ((0, 8),), -0.2, 0.2)), 0.05, 0.5)
    w_gate = centred(splits[9], (EXPERTS, D, FF), D ** -0.5, 0.09375, ((0, 8), (2, 2)))
    w_up = centred(splits[10], (EXPERTS, D, FF), D ** -0.5, 0.09375, ((0, 8), (2, 2)))
    w_down = centred(splits[11], (EXPERTS, FF, D), FF ** -0.5, 0.21875, ((0, 8), (1, 2)))
    return {"query": query, "latest_key_value": latest_key_value, "cache": cache, "lengths": lengths, "w_out": w_out, "residual_in": residual_in, "norm_gain": norm_gain, "expert_ids": expert_ids, "route_weights": route_weights, "w_gate": w_gate, "w_up": w_up, "w_down": w_down}


block_rows = 64

def attention(query, latest_key_value, cache, lengths):
    token_count = query.shape[0]
    kv_heads = latest_key_value.shape[2] // HEAD_SIZE
    group_size = query.shape[1] // (kv_heads * HEAD_SIZE)
    positions = cache.shape[2]
    factor = 1.0 / math.sqrt(HEAD_SIZE)
    queries = query.astype(jnp.float32).reshape(token_count, kv_heads, group_size, HEAD_SIZE)
    cached_keys = cache[:, 0].astype(jnp.float32).reshape(token_count, positions, kv_heads, HEAD_SIZE)
    cached_values = cache[:, 1].astype(jnp.float32).reshape(token_count, positions, kv_heads, HEAD_SIZE)
    fresh_keys = latest_key_value[:, 0].astype(jnp.float32).reshape(token_count, kv_heads, HEAD_SIZE)
    fresh_values = latest_key_value[:, 1].astype(jnp.float32).reshape(token_count, kv_heads, HEAD_SIZE)
    scores = jnp.einsum('tkgd,tlkd->tkgl', queries, cached_keys) * factor
    valid = jnp.arange(positions, dtype=jnp.int32)[None, :] < lengths[:, None]
    scores = jnp.where(valid[:, None, None, :], scores, -jnp.inf)
    own_score = jnp.einsum('tkgd,tkd->tkg', queries, fresh_keys) * factor
    highest = jnp.maximum(lax.optimization_barrier(jnp.max(scores, axis=-1)), own_score)
    weights = jnp.exp(scores - highest[..., None])
    own_weight = jnp.exp(own_score - highest)
    total = lax.optimization_barrier(jnp.sum(weights, axis=-1)) + own_weight
    probs = lax.optimization_barrier((weights / total[..., None]).astype(jnp.bfloat16))
    own_prob = lax.optimization_barrier((own_weight / total).astype(jnp.bfloat16))
    mixed = jnp.einsum('tkgl,tlkd->tkgd', probs.astype(jnp.float32), cached_values)
    mixed = mixed + own_prob.astype(jnp.float32)[..., None] * fresh_values[:, :, None, :]
    return mixed.reshape(token_count, -1).astype(jnp.bfloat16)

def reference(query, latest_key_value, cache, lengths, w_out, residual_in, norm_gain, expert_ids, route_weights, w_gate, w_up, w_down):
    attended = attention(query, latest_key_value, cache, lengths)
    stream = residual_in.astype(jnp.float32) + jnp.dot(attended, w_out, preferred_element_type=jnp.float32)
    meansq = lax.optimization_barrier(jnp.mean(stream * stream, axis=-1, keepdims=True))
    normed = (stream * lax.rsqrt(meansq + 1e-06) * norm_gain.astype(jnp.float32)).astype(jnp.bfloat16)
    assignments = REQUEST_TOTAL * TOP
    flat_ids = expert_ids.reshape(-1).astype(jnp.int32)
    sort_order = jnp.argsort(flat_ids, stable=True).astype(jnp.int32)
    sorted_ids = flat_ids[sort_order]
    expert_counts = lax.optimization_barrier(jnp.sum((flat_ids[:, None] == jnp.arange(EXPERTS, dtype=jnp.int32)[None, :]).astype(jnp.int32), axis=0))
    first_index = jnp.cumsum(expert_counts) - expert_counts
    rank_within = jnp.arange(assignments, dtype=jnp.int32) - first_index[sorted_ids]
    padded_counts = (expert_counts + block_rows - 1) // block_rows * block_rows
    padded_start = jnp.cumsum(padded_counts) - padded_counts
    position_sorted = (padded_start[sorted_ids] + rank_within).astype(jnp.int32)
    block_count = (assignments + block_rows - 1) // block_rows + EXPERTS
    position_of = jnp.zeros((assignments,), jnp.int32).at[sort_order].set(position_sorted)
    slot_token = jnp.zeros((block_count * block_rows,), jnp.int32).at[position_sorted].set(sort_order // TOP)
    block_starts = jnp.arange(block_count, dtype=jnp.int32) * block_rows
    block_expert = lax.optimization_barrier(jnp.sum((padded_start[None, :] <= block_starts[:, None]).astype(jnp.int32), axis=1)) - 1
    block_expert = jnp.clip(block_expert, 0, EXPERTS - 1).astype(jnp.int32)
    width_part = FF // N_TENSOR

    def run_block(block_index):
        chosen = block_expert[block_index]
        token_index = lax.dynamic_slice_in_dim(slot_token, block_index * block_rows, block_rows)
        inputs = normed[token_index]
        gate_proj = jnp.dot(inputs, w_gate[chosen], preferred_element_type=jnp.float32)
        up_proj = jnp.dot(inputs, w_up[chosen], preferred_element_type=jnp.float32)
        activated = (jax.nn.silu(gate_proj) * up_proj).astype(jnp.bfloat16)
        down_rows = w_down[chosen]
        summed = jnp.zeros((block_rows, D), jnp.float32)
        for piece in range(N_TENSOR):
            term = jnp.dot(activated[:, piece * width_part:(piece + 1) * width_part], down_rows[piece * width_part:(piece + 1) * width_part], preferred_element_type=jnp.float32)
            rounded = lax.optimization_barrier(term.astype(jnp.bfloat16))
            summed = summed + rounded.astype(jnp.float32)
        return summed.astype(jnp.bfloat16)
    outputs = lax.map(run_block, jnp.arange(block_count, dtype=jnp.int32)).reshape(block_count * block_rows, D)
    per_choice = outputs[position_of].astype(jnp.float32).reshape(REQUEST_TOTAL, TOP, D)
    mixture = lax.optimization_barrier(jnp.sum(route_weights.astype(jnp.float32)[:, :, None] * per_choice, axis=1))
    return (stream + mixture).astype(jnp.bfloat16)
```

```python
import math

import jax
import jax.numpy as jnp
from jax import lax
from jax.sharding import PartitionSpec as P

HEAD_SIZE = 128


def attention(query, latest_key_value, cache, lengths):
    token_count = query.shape[0]
    kv_heads = latest_key_value.shape[2] // HEAD_SIZE
    group_size = query.shape[1] // (kv_heads * HEAD_SIZE)
    positions = cache.shape[2]
    factor = 1.0 / math.sqrt(HEAD_SIZE)
    queries = query.reshape(token_count, kv_heads, group_size, HEAD_SIZE)
    cached_keys = cache[:, 0].reshape(token_count, positions, kv_heads, HEAD_SIZE)
    cached_values = cache[:, 1].reshape(token_count, positions, kv_heads, HEAD_SIZE)
    fresh_keys = latest_key_value[:, 0].reshape(token_count, kv_heads, HEAD_SIZE)
    fresh_values = (
        latest_key_value[:, 1].reshape(token_count, kv_heads, HEAD_SIZE).astype(jnp.float32)
    )
    scores = (
        jnp.einsum("tkgd,tlkd->tkgl", queries, cached_keys, preferred_element_type=jnp.float32)
        * factor
    )
    valid = jnp.arange(positions, dtype=jnp.int32)[None, :] < lengths[:, None]
    scores = jnp.where(valid[:, None, None, :], scores, -jnp.inf)
    own_score = (
        jnp.einsum("tkgd,tkd->tkg", queries, fresh_keys, preferred_element_type=jnp.float32)
        * factor
    )
    highest = jnp.maximum(jnp.max(scores, axis=-1), own_score)
    weights = jnp.exp(scores - highest[..., None])
    own_weight = jnp.exp(own_score - highest)
    total = jnp.sum(weights, axis=-1) + own_weight
    probs = (weights / total[..., None]).astype(jnp.bfloat16)
    own_prob = lax.optimization_barrier((own_weight / total).astype(jnp.bfloat16))
    mixed = jnp.einsum("tkgl,tlkd->tkgd", probs, cached_values, preferred_element_type=jnp.float32)
    mixed = mixed + own_prob.astype(jnp.float32)[..., None] * fresh_values[:, :, None, :]
    return mixed.reshape(token_count, -1).astype(jnp.bfloat16)


def per_device(
    query,
    latest_key_value,
    cache,
    lengths,
    w_out,
    residual_in,
    norm_gain,
    expert_ids,
    route_weights,
    w_gate,
    w_up,
    w_down,
):
    attended = attention(query, latest_key_value, cache, lengths)
    projected = jnp.dot(
        lax.all_gather(attended, "expert", axis=0, tiled=True),
        w_out,
        preferred_element_type=jnp.float32,
    )
    expert_groups = lax.axis_size("expert")
    token_count = query.shape[0]
    column_count = w_out.shape[1]
    grouped = projected.reshape(expert_groups, token_count, column_count)
    summed = lax.psum_scatter(
        grouped.astype(jnp.bfloat16), "tensor", scatter_dimension=1, tiled=True
    ).astype(jnp.float32)
    own_rows = lax.all_to_all(
        summed.astype(jnp.bfloat16), "expert", split_axis=0, concat_axis=2, tiled=True
    ).astype(summed.dtype)
    stream = residual_in.astype(jnp.float32) + own_rows.reshape(residual_in.shape)
    meansq = jnp.mean(stream * stream, axis=-1, keepdims=True)
    normed = (stream * lax.rsqrt(meansq + 1e-06) * norm_gain.astype(jnp.float32)).astype(
        jnp.bfloat16
    )
    local_experts = w_gate.shape[0]
    expert_total = local_experts * expert_groups
    named = expert_ids[:, :, None] == jnp.arange(expert_total, dtype=jnp.int32)[None, None, :]
    mixing = jnp.sum(jnp.where(named, route_weights[:, :, None], 0.0), axis=1)
    mixing = lax.all_to_all(
        mixing.reshape(token_count, expert_groups, local_experts),
        "expert",
        split_axis=1,
        concat_axis=0,
        tiled=True,
    ).reshape(token_count * expert_groups, local_experts)
    whole_rows = lax.all_gather(normed, ("expert", "tensor"), axis=0, tiled=True)
    pieces = []
    for x in range(local_experts):
        gate_proj = jnp.dot(whole_rows, w_gate[x], preferred_element_type=jnp.float32)
        up_proj = jnp.dot(whole_rows, w_up[x], preferred_element_type=jnp.float32)
        activated = jax.nn.silu(gate_proj) * up_proj * mixing[:, x][:, None]
        pieces.append(activated.astype(jnp.bfloat16))
    partial_out = jnp.dot(
        jnp.concatenate(pieces, axis=1),
        w_down.reshape(-1, w_down.shape[2]),
        preferred_element_type=jnp.float32,
    )
    mixture_rows = lax.psum_scatter(
        partial_out.astype(jnp.bfloat16), ("expert", "tensor"), scatter_dimension=0, tiled=True
    )
    return (stream + mixture_rows.astype(jnp.float32)).astype(jnp.bfloat16)


def solution(mesh):
    placed = (
        P(("groups", "expert"), "tensor"),
        P(("groups", "expert"), None, "tensor"),
        P(("groups", "expert"), None, None, "tensor"),
        P(("groups", "expert")),
        P("tensor", "expert"),
        P(("groups", "expert", "tensor"), None),
        P(),
        P(("groups", "expert"), None),
        P(("groups", "expert"), None),
        P("expert", None, "tensor"),
        P("expert", None, "tensor"),
        P("expert", "tensor", None),
    )
    return jax.shard_map(
        per_device,
        mesh=mesh,
        in_specs=placed,
        out_specs=P(("groups", "expert", "tensor"), None),
        check_vma=False,
    )
```

```python
import functools
import math

import jax
import jax.numpy as jnp
from jax import lax
from jax.experimental import pallas as pl
from jax.experimental.pallas import tpu as pltpu
from jax.sharding import PartitionSpec as P

HEAD_SIZE = 128


def attention(query, latest_key_value, cache, lengths):
    token_count = query.shape[0]
    kv_heads = latest_key_value.shape[2] // HEAD_SIZE
    group_size = query.shape[1] // (kv_heads * HEAD_SIZE)
    positions = cache.shape[2]
    factor = 1.0 / math.sqrt(HEAD_SIZE)
    queries = query.reshape(token_count, kv_heads, group_size, HEAD_SIZE)
    cached_keys = cache[:, 0].reshape(token_count, positions, kv_heads, HEAD_SIZE)
    cached_values = cache[:, 1].reshape(token_count, positions, kv_heads, HEAD_SIZE)
    fresh_keys = latest_key_value[:, 0].reshape(token_count, kv_heads, HEAD_SIZE)
    fresh_values = (
        latest_key_value[:, 1].reshape(token_count, kv_heads, HEAD_SIZE).astype(jnp.float32)
    )
    scores = (
        jnp.einsum("tkgd,tlkd->tkgl", queries, cached_keys, preferred_element_type=jnp.float32)
        * factor
    )
    valid = jnp.arange(positions, dtype=jnp.int32)[None, :] < lengths[:, None]
    scores = jnp.where(valid[:, None, None, :], scores, -jnp.inf)
    own_score = (
        jnp.einsum("tkgd,tkd->tkg", queries, fresh_keys, preferred_element_type=jnp.float32)
        * factor
    )
    highest = jnp.maximum(jnp.max(scores, axis=-1), own_score)
    weights = jnp.exp(scores - highest[..., None])
    own_weight = jnp.exp(own_score - highest)
    total = jnp.sum(weights, axis=-1) + own_weight
    probs = (weights / total[..., None]).astype(jnp.bfloat16)
    own_prob = lax.optimization_barrier((own_weight / total).astype(jnp.bfloat16))
    mixed = jnp.einsum("tkgl,tlkd->tkgd", probs, cached_values, preferred_element_type=jnp.float32)
    mixed = mixed + own_prob.astype(jnp.float32)[..., None] * fresh_values[:, :, None, :]
    return mixed.reshape(token_count, -1).astype(jnp.bfloat16)


CORES = 2
MESH = pl.DeviceIdType.MESH
DMA = pltpu.SemaphoreType.DMA
VMEM_SPEC = pl.BlockSpec(memory_space=pltpu.VMEM)


def remote(src, dst, send_sem, recv_sem, **device):
    return pltpu.make_async_remote_copy(
        src_ref=src,
        dst_ref=dst,
        send_sem=send_sem,
        recv_sem=recv_sem,
        device_id=device,
        device_id_type=MESH,
    )


class Place:
    def __init__(self, chips, groups):
        self.chips, self.groups = chips, groups
        self.expert = lax.axis_index("expert")
        self.tensor = lax.axis_index("tensor")
        self.chip, self.core = self.expert // CORES, self.expert % CORES
        self.partner = self.chip * CORES + 1 - self.core

    def inside(self, chip):
        return jnp.logical_and(chip >= 0, chip < self.chips)

    def greet_line(self, barrier):
        pl.semaphore_signal(barrier, 1, device_id={"expert": self.partner}, device_id_type=MESH)
        for step in (-1, 1):

            @pl.when(self.inside(self.chip + step))
            def _():
                pl.semaphore_signal(
                    barrier,
                    1,
                    device_id={"expert": self.expert + CORES * step},
                    device_id_type=MESH,
                )

        ends = (self.chip == 0).astype(jnp.int32) + (self.chip == self.chips - 1).astype(jnp.int32)
        return 3 - ends

    def greet_tensor(self, barrier):
        for shift in range(1, self.groups):
            other = (self.tensor + shift) % self.groups
            pl.semaphore_signal(barrier, 1, device_id={"tensor": other}, device_id_type=MESH)
        return self.groups - 1


def line_gather(place, arrays, sems, slot, across):
    line_send, line_recv, core_send, core_recv, cross_send, cross_recv = sems
    chips, core = place.chips, place.core
    groups = place.groups if across else 1
    waits = []

    def block(a, chip, tensor, own):
        source, whole = arrays[a]
        if own:
            return source
        return whole.at[slot(chip * CORES + core, tensor)]

    def landing(a, chip, tensor, of_core):
        return arrays[a][1].at[slot(chip * CORES + of_core, tensor)]

    def line(a, side, step, chip, own):
        way = 1 - 2 * side
        return remote(
            block(a, chip, place.tensor, own),
            landing(a, chip, place.tensor, core),
            line_send.at[a, side, step],
            line_recv.at[a, side, step + 1],
            expert=place.expert + CORES * way,
        )

    def line_arrival(a, side, step, chip):
        here = landing(a, chip, place.tensor, core)
        return remote(here, here, line_send.at[a, side, step], line_recv.at[a, side, step],
                      expert=place.partner)

    def to_partner(a, shift, chip, own):
        tensor = (place.tensor + shift) % place.groups
        return remote(
            block(a, chip, tensor, own),
            landing(a, chip, tensor, core),
            core_send.at[a, shift, chip],
            core_recv.at[a, shift, chip],
            expert=place.partner,
        )

    def partner_arrival(a, shift, chip):
        tensor = (place.tensor + shift) % place.groups
        here = landing(a, chip, tensor, 1 - core)
        return remote(here, here, core_send.at[a, shift, chip], core_recv.at[a, shift, chip],
                      expert=place.partner)

    def cross(a, shift, chip, own):
        other = (place.tensor + shift) % place.groups
        return remote(
            block(a, chip, place.tensor, own),
            landing(a, chip, place.tensor, core),
            cross_send.at[a, shift, chip],
            cross_recv.at[a, shift, chip],
            tensor=other,
        )

    def cross_arrival(a, shift, chip):
        tensor = (place.tensor + place.groups - shift) % place.groups
        here = landing(a, chip, tensor, core)
        return remote(here, here, cross_send.at[a, shift, chip], cross_recv.at[a, shift, chip],
                      expert=place.partner)

    count = len(arrays)

    def hand_on(step, side, chip):
        own = step == 0
        way = 1 - 2 * side

        @pl.when(place.inside(chip))
        def _():
            if not own:
                for a in range(count):
                    line_arrival(a, side, step, chip).wait_recv()

            @pl.when(place.inside(place.chip + way))
            def _():
                for a in range(count):
                    line(a, side, step, chip, own).start()

            if not own or side == 0:
                for a in range(count):
                    for shift in range(1, groups):
                        cross(a, shift, chip, own).start()
                    to_partner(a, 0, chip, own).start()

    def hand_on_crossed(step, side, chip):
        if step == 0 and side == 1:
            return

        @pl.when(place.inside(chip))
        def _():
            for a in range(count):
                for shift in range(1, groups):
                    cross_arrival(a, shift, chip).wait_recv()
                    to_partner(a, place.groups - shift, chip, False).start()

    sides = [(side, step) for step in range(chips) for side in range(2)]
    chip_at = lambda side, step: place.chip - (1 - 2 * side) * step
    for step in range(chips):
        for side in range(2):
            hand_on(step, side, chip_at(side, step))
        if step > 0 and groups > 1:
            for side in range(2):
                hand_on_crossed(step - 1, side, chip_at(side, step - 1))
    if groups > 1:
        for side in range(2):
            hand_on_crossed(chips - 1, side, chip_at(side, chips - 1))
    for chip in range(chips):
        for shift in range(groups):
            for a in range(count):
                partner_arrival(a, shift, chip).wait_recv()
    for side, step in sides:
        own = step == 0
        chip = chip_at(side, step)

        @pl.when(jnp.logical_and(place.inside(chip), place.inside(place.chip + 1 - 2 * side)))
        def _():
            for a in range(count):
                line(a, side, step, chip, own).wait_send()

    for a in range(count):
        for shift in range(groups):
            for chip in range(chips):
                partner_arrival(a, shift, chip).wait_send()
                if shift:
                    cross_arrival(a, shift, chip).wait_send()


def gather_sems(count, chips, groups):
    return [
        DMA((count, 2, chips)),
        DMA((count, 2, chips + 1)),
        DMA((count, groups, chips)),
        DMA((count, groups, chips)),
        DMA((count, groups, chips)),
        DMA((count, groups, chips)),
    ]


def attended_kernel(chips, groups, rows, weights, all_rows, all_weights, own_sem, *sems):
    place = Place(chips, groups)
    barrier = pltpu.get_barrier_semaphore()
    pl.semaphore_wait(barrier, place.greet_line(barrier))
    keep = [
        pltpu.make_async_copy(rows, all_rows.at[place.expert], own_sem.at[0]),
        pltpu.make_async_copy(weights, all_weights.at[place.expert], own_sem.at[1]),
    ]
    for copy in keep:
        copy.start()
    line_gather(
        place,
        [(rows, all_rows), (weights, all_weights)],
        sems,
        lambda expert, tensor: expert,
        False,
    )
    for copy in keep:
        copy.wait()


def gather_attended(rows, weights, groups):
    experts = lax.axis_size("expert")
    chips = experts // CORES
    return pl.pallas_call(
        functools.partial(attended_kernel, chips, groups),
        out_shape=[
            jax.ShapeDtypeStruct((experts,) + rows.shape, rows.dtype),
            jax.ShapeDtypeStruct((experts,) + weights.shape, weights.dtype),
        ],
        in_specs=[VMEM_SPEC] * 2,
        out_specs=[VMEM_SPEC] * 2,
        scratch_shapes=[DMA((2,))] + gather_sems(2, chips, groups),
        compiler_params=pltpu.CompilerParams(collective_id=0, has_side_effects=True),
    )(rows, weights)


def stream_kernel(
    chips, groups, projected, residual, gain, stream, normed, own, crossed, summed, arrived,
    swap_send, swap_recv, out_send, out_recv, *sems
):
    place = Place(chips, groups)
    experts = chips * CORES
    barrier = pltpu.get_barrier_semaphore()
    for shift in range(1, experts):
        other = (place.expert + shift) % experts
        pl.semaphore_signal(barrier, 1, device_id={"expert": other}, device_id_type=MESH)
    pl.semaphore_wait(barrier, experts - 1 + place.greet_tensor(barrier))

    def swap(shift):
        other = (place.tensor + shift) % groups
        return remote(
            projected.at[other],
            crossed.at[shift - 1],
            swap_send.at[shift - 1],
            swap_recv.at[shift - 1],
            tensor=other,
        )

    def hand_out(shift):
        other = (place.expert + shift) % experts
        return remote(
            summed.at[other],
            arrived.at[shift],
            out_send.at[shift],
            out_recv.at[shift],
            expert=other,
        )

    for shift in range(1, groups):
        swap(shift).start()
    for shift in range(1, groups):
        swap(shift).wait()
    for shift in list(range(1, experts)) + [0]:
        expert = (place.expert + shift) % experts
        total = projected[place.tensor, expert].astype(jnp.float32)
        for other in range(groups - 1):
            total = total + crossed[other, expert].astype(jnp.float32)
        summed[expert] = total.astype(jnp.bfloat16)
        if shift:
            hand_out(shift).start()
    for shift in range(1, experts):
        hand_out(shift).wait()
    arrived[0] = summed[place.expert]
    width = stream.shape[1] // experts
    square = 0.0
    for expert in range(experts):
        columns = pl.ds(expert * width, width)
        shift = (place.expert - expert + experts) % experts
        part = residual[:, columns].astype(jnp.float32) + arrived[shift].astype(jnp.float32)
        stream[:, columns] = part
        square = square + jnp.sum(part * part, axis=1, keepdims=True)
    scale = lax.rsqrt(square * (1.0 / stream.shape[1]) + 1e-06)
    for expert in range(experts):
        columns = pl.ds(expert * width, width)
        value = stream[:, columns] * scale * gain[:, columns].astype(jnp.float32)
        own[:, columns] = value.astype(jnp.bfloat16)
    mine = place.expert * groups + place.tensor
    normed[mine] = own[...]
    line_gather(
        place, [(own, normed)], sems, lambda expert, tensor: expert * groups + tensor, True
    )


def exchange_stream(projected, residual, gain):
    groups, experts, rows, width = projected.shape
    chips = experts // CORES
    model = residual.shape[1]
    return pl.pallas_call(
        functools.partial(stream_kernel, chips, groups),
        out_shape=[
            jax.ShapeDtypeStruct((rows, model), jnp.float32),
            jax.ShapeDtypeStruct((experts * groups, rows, model), jnp.bfloat16),
        ],
        in_specs=[VMEM_SPEC] * 3,
        out_specs=[VMEM_SPEC] * 2,
        scratch_shapes=[
            pltpu.VMEM((rows, model), jnp.bfloat16),
            pltpu.VMEM((max(groups - 1, 1), experts, rows, width), jnp.bfloat16),
            pltpu.VMEM((experts, rows, width), jnp.bfloat16),
            pltpu.VMEM((experts, rows, width), jnp.bfloat16),
            DMA((groups,)),
            DMA((groups,)),
            DMA((experts,)),
            DMA((experts,)),
        ]
        + gather_sems(1, chips, groups),
        compiler_params=pltpu.CompilerParams(collective_id=1, has_side_effects=True),
    )(projected, residual, gain)


def scatter_kernel(
    chips, groups, partial, total, core_in, crossing, cross_in, sums, line_in,
    core_send, core_recv, cross_send, cross_recv, line_send, line_recv
):
    place = Place(chips, groups)
    chip, core, tensor = place.chip, place.core, place.tensor
    barrier = pltpu.get_barrier_semaphore()
    peers = place.greet_line(barrier) + place.greet_tensor(barrier)
    pl.semaphore_wait(barrier, peers)

    def target(m):
        low = jnp.where(m < chips - 1 - chip, chips - 1 - m, m - (chips - 1 - chip))
        high = jnp.where(m < chip, m, chips - 1 - (m - chip))
        return jnp.where(chip * 2 < chips, low, high)

    def to_partner(m, shift):
        j, t = target(m), (tensor + shift) % groups
        return remote(
            partial.at[(j * CORES + 1 - core) * groups + t],
            core_in.at[j * groups + t],
            core_send.at[m, shift],
            core_recv.at[m, shift],
            expert=place.partner,
        )

    def cross(m, shift):
        j = target(m)
        return remote(
            crossing.at[shift - 1, j],
            cross_in.at[shift - 1, j],
            cross_send.at[m, shift],
            cross_recv.at[m, shift],
            tensor=(tensor + shift) % groups,
        )

    def pair_sum(m, shift):
        j, t = target(m), (tensor + shift) % groups
        mine = partial[(j * CORES + core) * groups + t].astype(jnp.float32)
        return mine + core_in[j * groups + t].astype(jnp.float32)

    for shift in list(range(1, groups)) + [0]:
        for m in range(chips):
            to_partner(m, shift).start()
    for m in range(chips):
        for shift in range(1, groups):
            to_partner(m, shift).wait_recv()
            crossing[shift - 1, target(m)] = pair_sum(m, shift).astype(jnp.bfloat16)
            cross(m, shift).start()

    def along(j, side):
        way = 1 - 2 * side
        return remote(
            sums.at[j],
            line_in.at[side, j],
            line_send.at[j],
            line_recv.at[side, j],
            expert=place.expert + CORES * way,
        )

    def line_arrival(j, side):
        return remote(line_in.at[side, j], line_in.at[side, j], line_send.at[j],
                      line_recv.at[side, j], expert=place.partner)

    for m in range(chips):
        j = target(m)
        to_partner(m, 0).wait_recv()
        value = pair_sum(m, 0)
        for shift in range(1, groups):
            cross(m, shift).wait_recv()
            value = value + cross_in[shift - 1, j].astype(jnp.float32)
        if m < chips - 1:
            for side in range(2):
                ahead = j > chip if side == 0 else j < chip
                source = place.inside(chip - (1 - 2 * side))

                @pl.when(jnp.logical_and(ahead, source))
                def _():
                    line_arrival(j, side).wait_recv()
                    sums[j] = (value + line_in[side, j].astype(jnp.float32)).astype(jnp.bfloat16)
                    along(j, side).start()

                @pl.when(jnp.logical_and(ahead, jnp.logical_not(source)))
                def _():
                    sums[j] = value.astype(jnp.bfloat16)
                    along(j, side).start()

        else:
            total[...] = value
            for side in range(2):

                @pl.when(place.inside(chip - (1 - 2 * side)))
                def _():
                    line_arrival(j, side).wait_recv()
                    total[...] += line_in[side, j].astype(jnp.float32)

    for m in range(chips):
        for shift in range(groups):
            to_partner(m, shift).wait_send()
            if shift:
                cross(m, shift).wait_send()
        if m < chips - 1:
            line_arrival(target(m), 0).wait_send()


def scatter_sum(partial, groups):
    blocks, rows, model = partial.shape
    experts = blocks // groups
    chips = experts // CORES
    block = (rows, model)
    others = max(groups - 1, 1)
    return pl.pallas_call(
        functools.partial(scatter_kernel, chips, groups),
        out_shape=jax.ShapeDtypeStruct(block, jnp.float32),
        in_specs=[VMEM_SPEC],
        out_specs=VMEM_SPEC,
        scratch_shapes=[
            pltpu.VMEM((chips * groups,) + block, jnp.bfloat16),
            pltpu.VMEM((others, chips) + block, jnp.bfloat16),
            pltpu.VMEM((others, chips) + block, jnp.bfloat16),
            pltpu.VMEM((chips,) + block, jnp.bfloat16),
            pltpu.VMEM((2, chips) + block, jnp.bfloat16),
        ]
        + [DMA((chips, groups))] * 4
        + [DMA((chips,)), DMA((2, chips))],
        compiler_params=pltpu.CompilerParams(collective_id=2, has_side_effects=True),
    )(partial)


def route_table(expert_ids, route_weights, expert_total):
    named = expert_ids[:, :, None] == jnp.arange(expert_total, dtype=jnp.int32)[None, None, :]
    return jnp.sum(jnp.where(named, route_weights[:, :, None], 0.0), axis=1)


def experts_sum(whole_rows, mixing, w_gate, w_up, w_down):
    pieces = []
    for x in range(w_gate.shape[0]):
        gate_proj = jnp.dot(whole_rows, w_gate[x], preferred_element_type=jnp.float32)
        up_proj = jnp.dot(whole_rows, w_up[x], preferred_element_type=jnp.float32)
        activated = jax.nn.silu(gate_proj) * up_proj * mixing[:, x][:, None]
        pieces.append(activated.astype(jnp.bfloat16))
    return jnp.dot(
        jnp.concatenate(pieces, axis=1),
        w_down.reshape(-1, w_down.shape[2]),
        preferred_element_type=jnp.float32,
    ).astype(jnp.bfloat16)


def with_kernels(
    query,
    latest_key_value,
    cache,
    lengths,
    w_out,
    residual_in,
    norm_gain,
    expert_ids,
    route_weights,
    w_gate,
    w_up,
    w_down,
):
    experts, groups = lax.axis_size("expert"), lax.axis_size("tensor")
    local_experts = w_gate.shape[0]
    expert_total = local_experts * experts
    rows, model = residual_in.shape
    table = route_table(expert_ids, route_weights, expert_total)
    high = table.astype(jnp.bfloat16)
    low = (table - high.astype(jnp.float32)).astype(jnp.bfloat16)
    pair = jnp.concatenate([high, low], axis=1)
    pair = jnp.pad(pair, ((0, 0), (0, -pair.shape[1] % 128)))
    attended = attention(query, latest_key_value, cache, lengths)
    all_attended, all_pairs = gather_attended(attended, pair, groups)
    all_pairs = all_pairs.reshape(-1, pair.shape[1]).astype(jnp.float32)
    tables = all_pairs[:, :expert_total] + all_pairs[:, expert_total : 2 * expert_total]
    mixing = lax.dynamic_slice_in_dim(
        tables, lax.axis_index("expert") * local_experts, local_experts, axis=1
    )
    projected = jnp.dot(
        all_attended.reshape(-1, attended.shape[1]), w_out, preferred_element_type=jnp.float32
    ).astype(jnp.bfloat16)
    projected = projected.reshape(experts, groups, rows, -1).swapaxes(0, 1)
    stream, normed = exchange_stream(projected, residual_in, norm_gain.reshape(1, model))
    partial_out = experts_sum(normed.reshape(-1, model), mixing, w_gate, w_up, w_down)
    mixture = scatter_sum(partial_out.reshape(experts * groups, rows, model), groups)
    return (stream + mixture).astype(jnp.bfloat16)


def with_collectives(
    query,
    latest_key_value,
    cache,
    lengths,
    w_out,
    residual_in,
    norm_gain,
    expert_ids,
    route_weights,
    w_gate,
    w_up,
    w_down,
):
    attended = attention(query, latest_key_value, cache, lengths)
    projected = jnp.dot(
        lax.all_gather(attended, "expert", axis=0, tiled=True),
        w_out,
        preferred_element_type=jnp.float32,
    )
    expert_groups = lax.axis_size("expert")
    token_count = query.shape[0]
    column_count = w_out.shape[1]
    grouped = projected.reshape(expert_groups, token_count, column_count)
    summed = lax.psum_scatter(
        grouped.astype(jnp.bfloat16), "tensor", scatter_dimension=1, tiled=True
    ).astype(jnp.float32)
    own_rows = lax.all_to_all(
        summed.astype(jnp.bfloat16), "expert", split_axis=0, concat_axis=2, tiled=True
    ).astype(summed.dtype)
    stream = residual_in.astype(jnp.float32) + own_rows.reshape(residual_in.shape)
    meansq = jnp.mean(stream * stream, axis=-1, keepdims=True)
    normed = (stream * lax.rsqrt(meansq + 1e-06) * norm_gain.astype(jnp.float32)).astype(
        jnp.bfloat16
    )
    local_experts = w_gate.shape[0]
    expert_total = local_experts * expert_groups
    named = expert_ids[:, :, None] == jnp.arange(expert_total, dtype=jnp.int32)[None, None, :]
    mixing = jnp.sum(jnp.where(named, route_weights[:, :, None], 0.0), axis=1)
    mixing = lax.all_to_all(
        mixing.reshape(token_count, expert_groups, local_experts),
        "expert",
        split_axis=1,
        concat_axis=0,
        tiled=True,
    ).reshape(token_count * expert_groups, local_experts)
    whole_rows = lax.all_gather(normed, ("expert", "tensor"), axis=0, tiled=True)
    pieces = []
    for x in range(local_experts):
        gate_proj = jnp.dot(whole_rows, w_gate[x], preferred_element_type=jnp.float32)
        up_proj = jnp.dot(whole_rows, w_up[x], preferred_element_type=jnp.float32)
        activated = jax.nn.silu(gate_proj) * up_proj * mixing[:, x][:, None]
        pieces.append(activated.astype(jnp.bfloat16))
    partial_out = jnp.dot(
        jnp.concatenate(pieces, axis=1),
        w_down.reshape(-1, w_down.shape[2]),
        preferred_element_type=jnp.float32,
    )
    mixture_rows = lax.psum_scatter(
        partial_out.astype(jnp.bfloat16), ("expert", "tensor"), scatter_dimension=0, tiled=True
    )
    return (stream + mixture_rows.astype(jnp.float32)).astype(jnp.bfloat16)


def solution(mesh):
    placed = (
        P(("groups", "expert"), "tensor"),
        P(("groups", "expert"), None, "tensor"),
        P(("groups", "expert"), None, None, "tensor"),
        P(("groups", "expert")),
        P("tensor", "expert"),
        P(("groups", "expert", "tensor"), None),
        P(),
        P(("groups", "expert"), None),
        P(("groups", "expert"), None),
        P("expert", None, "tensor"),
        P("expert", None, "tensor"),
        P("expert", "tensor", None),
    )

    def per_device(*arrays):
        rows, columns = arrays[5].shape[0], arrays[4].shape[1]
        whole_tiles = rows % 8 == 0 and columns % 128 == 0
        paired = mesh.shape["expert"] % CORES == 0
        return (with_kernels if whole_tiles and paired else with_collectives)(*arrays)

    return jax.shard_map(
        per_device,
        mesh=mesh,
        in_specs=placed,
        out_specs=P(("groups", "expert", "tensor"), None),
        check_vma=False,
    )
```
